32 devices in a mesh: lat: 8 (over z, x), lev: 4 (over y, core).
Axes of the slice: x: 2, y: 2, z: 4, core: 2. Of those that a mesh axis runs over, the one named last changes fastest.
Arguments:
- fourier: bfloat16 [1280, 640, 1024], P('lat', None, 'lev'), may hold values from -6 to 6
- legendre: bfloat16 [640, 2, 640, 320], P('lat', None, 'lev'), may hold values from -0.25 to 0.25
- owner: int32 [640], replicated, may hold values from 0 to 7, as said below
Outputs:
- spectral: bfloat16 [640, 2, 320, 1024], P('lat', None, None, 'lev')
The draws below stay inside these ranges and needn't reach their ends.
Inputs may be any that keep to these rules, and one draw needn't show every extreme that they name: `owner`: each index along lat is named by exactly 80 wavenumbers.
All inputs are finite; a program needn't handle non-finite values.
Results may differ from the reference program's by a relative error of at most 0.0051.
Values may be sent and summed in bfloat16 or wider, within the bound.
A program may use at most 384 MiB of HBM per device.

```python
import jax
import jax.numpy as jnp
from jax import lax

M = 640
NLAT = 1280
COLS = 1024
NH = 640
HALF = 320
SLOTS = 80
N_LAT = 8


def draw_owner(key, part):
    jitter_key = jax.random.fold_in(key, 101)
    device_key = jax.random.fold_in(key, 202)
    wave_ids = jnp.arange(M, dtype=jnp.int32)
    jitter = jax.random.randint(jitter_key, (M,), 0, 4 * SLOTS, dtype=jnp.int32)
    scores = (wave_ids + jitter) * M + wave_ids
    ordering = jnp.argsort(scores, stable=True).astype(jnp.int32)
    ranking = jnp.argsort(ordering, stable=True).astype(jnp.int32)
    devices = jax.random.permutation(device_key, M // SLOTS).astype(jnp.int32)
    return devices[ranking // SLOTS]


def levels(own_key, extent, split, smallest, high):
    def one(axis_at, shards_of):
        draws = jax.random.uniform(jax.random.fold_in(jax.random.fold_in(own_key, 6), axis_at), (shards_of,), jnp.float32, smallest / len(split), high / len(split))
        return jnp.repeat(jnp.exp(draws), extent[axis_at] // shards_of).reshape((-1,) + (1,) * (len(extent) - axis_at - 1))

    level = one(*split[0])
    for cut in split[1:]:
        level = level * one(*cut)
    return level


def bell_draw(key, dims, scale, reach, shards=(), kind=jnp.bfloat16):
    result = jax.random.normal(key, dims, jnp.float32) * scale
    if len(shards) > 0:
        result = levels(key, dims, shards, -0.22, 0.18) * result
    return jnp.clip(result, min=-reach, max=reach).astype(kind)


def setup_inputs(seed: int = 0) -> dict:
    arg_keys = jax.random.split(jax.random.key(seed), 4)
    fourier = bell_draw(arg_keys[0], (NLAT, M, COLS), 1.0, 6.0, ((0, 8), (2, 4)))
    legendre = bell_draw(arg_keys[1], (M, 2, NH, HALF), NH ** -0.5, 0.25, ((0, 8), (2, 4)))
    owner = draw_owner(jax.random.fold_in(arg_keys[3], 71), 0)
    return {"fourier": fourier, "legendre": legendre, "owner": owner}


def slot_waves(owner, slot_count):
    wave_count = owner.shape[0]
    wave_ids = jnp.arange(wave_count, dtype=jnp.int32)
    earlier = (owner[None, :] == owner[:, None]) & (wave_ids[None, :] < wave_ids[:, None])
    ranked = jnp.sum(earlier.astype(jnp.int32), axis=1)
    placed = owner * slot_count + ranked
    matched = placed[None, :] == wave_ids[:, None]
    return jnp.sum(jnp.where(matched, wave_ids[None, :], 0), axis=1).astype(jnp.int32)


def reference(fourier, legendre, owner):
    wave_of = slot_waves(owner, M // N_LAT)
    north_count = NLAT // 2
    degree = jnp.arange(M // 2, dtype=jnp.int32)
    parities = jnp.arange(2, dtype=jnp.int32)

    def one_slot(operands):
        wave, table_part = operands
        column = lax.dynamic_index_in_dim(fourier, wave, axis=1, keepdims=False)
        upper_rows = column[:north_count].astype(jnp.float32)
        lower_rows = column[north_count:].astype(jnp.float32)
        even_rows = (upper_rows + lower_rows).astype(jnp.bfloat16)
        odd_rows = (upper_rows - lower_rows).astype(jnp.bfloat16)
        even_out = jnp.dot(table_part[0].T, even_rows, preferred_element_type=jnp.float32)
        odd_out = jnp.dot(table_part[1].T, odd_rows, preferred_element_type=jnp.float32)
        live_count = (M - wave - parities + 1) // 2
        kept_mask = degree[None, :] < live_count[:, None]
        stacked = jnp.stack([even_out, odd_out])
        return jnp.where(kept_mask[:, :, None], stacked, 0.0).astype(jnp.bfloat16)

    return lax.map(one_slot, (wave_of, legendre))
```

```python
import functools

import jax
import jax.numpy as jnp
from jax import lax
from jax.experimental import pallas as pl
from jax.experimental.pallas import tpu as pltpu
from jax.sharding import PartitionSpec as P

CHUNKS = 2
GROUP = 8
PIECE = 2
ROWS = 16


def ranks(owner, slot_count):
    wave_count = owner.shape[0]
    wave_ids = jnp.arange(wave_count, dtype=jnp.int32)
    earlier = (owner[None, :] == owner[:, None]) & (wave_ids[None, :] < wave_ids[:, None])
    ranked = jnp.sum(earlier.astype(jnp.int32), axis=1)
    return owner * slot_count + ranked


def flipped(index, mask):
    bit = 1
    result = index
    while bit <= mask:
        if mask & bit:
            result = result + bit * (1 - 2 * lax.rem(lax.div(index, bit), 2))
        bit *= 2
    return result


def far_first(count):
    half = count // 2
    far = [half + m for m in range(half)]
    near = [m for m in range(1, half)]
    order = sorted(far, key=lambda m: (m & 1, -m)) + sorted(near, key=lambda m: (m == 1, m))
    return order


def exchange(
    fourier_ref, picks_ref, table_ref,
    out_ref, send_ref, land_ref, tables_ref,
    block, drawn, packed, rows, table, made, even, odd,
    block_sem, packed_sem, send_first, recv_first, send_sem, recv_sem,
    table_send, table_recv, load_sem, store_sem,
):
    lat_count, slot_count, row_count, column_count = send_ref.shape
    half_rows = table_ref.shape[3]
    lev_count = tables_ref.shape[0] + 1
    chunks = slot_count // GROUP
    blocks = row_count // ROWS
    pieces = GROUP // PIECE
    me, lev = lax.axis_index("lat"), lax.axis_index("lev")
    order = far_first(lat_count)
    peers = {m: (flipped(me, m), lev) for m in order}
    sides = {m: (me, flipped(lev, m)) for m in range(1, lev_count)}
    mesh_ids = pl.DeviceIdType.MESH

    barrier = pltpu.get_barrier_semaphore()
    for peer in [*peers.values(), *sides.values()]:
        pl.semaphore_signal(barrier, inc=1, device_id=peer, device_id_type=mesh_ids)
    pl.semaphore_wait(barrier, len(peers) + len(sides))

    def table_copy(chunk, mask):
        span = pl.ds(chunk * GROUP, GROUP)
        return pltpu.make_async_remote_copy(
            src_ref=table_ref.at[span], dst_ref=tables_ref.at[mask - 1, span],
            send_sem=table_send.at[chunk, mask - 1], recv_sem=table_recv.at[chunk, mask - 1],
            device_id=sides[mask], device_id_type=mesh_ids,
        )

    def first_copy(step, mask):
        span = (pl.ds(0, GROUP), pl.ds(step * ROWS, ROWS))
        return pltpu.make_async_remote_copy(
            src_ref=send_ref.at[(mask, *span)], dst_ref=land_ref.at[(mask - 1, *span)],
            send_sem=send_first.at[step, mask - 1], recv_sem=recv_first.at[step, mask - 1],
            device_id=peers[mask], device_id_type=mesh_ids,
        )

    def later_copy(piece, mask):
        span = pl.ds(piece * PIECE, PIECE)
        return pltpu.make_async_remote_copy(
            src_ref=send_ref.at[mask, span], dst_ref=land_ref.at[mask - 1, span],
            send_sem=send_sem.at[piece, mask - 1], recv_sem=recv_sem.at[piece, mask - 1],
            device_id=peers[mask], device_id_type=mesh_ids,
        )

    def block_copy(step, side):
        return pltpu.make_async_copy(
            fourier_ref.at[pl.ds(step * ROWS, ROWS)], block.at[side], block_sem.at[side]
        )

    def pick(chunk, after):
        block_copy(0, 0).start()

        def one(step, carry):
            side = lax.rem(step, 2)

            @pl.when(step + 1 < blocks)
            def _():
                block_copy(step + 1, 1 - side).start()

            block_copy(step, side).wait()

            def row(r, inner):
                drawn[:, r, :] = jnp.dot(
                    picks_ref[chunk], block[side, r], preferred_element_type=jnp.float32
                )
                return inner

            for r in range(ROWS):
                row(r, 0)
            packed[...] = drawn[...].astype(packed.dtype).reshape(packed.shape)
            copy = pltpu.make_async_copy(
                packed,
                send_ref.at[:, pl.ds(chunk * GROUP, GROUP), pl.ds(step * ROWS, ROWS)],
                packed_sem,
            )
            copy.start()
            copy.wait()
            after(step)
            return carry

        lax.fori_loop(0, blocks, one, 0)

    def project(piece):
        span = pl.ds(piece * PIECE, PIECE)
        copies = [pltpu.make_async_copy(send_ref.at[0, span], rows.at[:, me], load_sem.at[0])]
        for m in order:
            copies.append(pltpu.make_async_copy(
                land_ref.at[m - 1, span], rows.at[:, peers[m][0]], load_sem.at[m]))
        for m in range(lev_count):
            source = table_ref.at[span] if m == 0 else tables_ref.at[m - 1, span]
            start = pl.multiple_of((lev if m == 0 else sides[m][1]) * row_count, ROWS)
            copies.append(pltpu.make_async_copy(
                source, table.at[:, :, pl.ds(start, row_count)], load_sem.at[lat_count + m]))
        for copy in copies:
            copy.start()
        for copy in copies:
            copy.wait()

        def one(i, carry):
            half = lat_count // 2
            upper = rows[i, :half].astype(jnp.float32).reshape(-1, column_count)
            lower = rows[i, half:].astype(jnp.float32).reshape(-1, column_count)
            even[...] = (upper + lower).astype(even.dtype)
            odd[...] = (upper - lower).astype(odd.dtype)
            for parity, part in enumerate((even, odd)):
                total = lax.dot_general(
                    table[i, parity], part[...], (((0,), (0,)), ((), ())),
                    preferred_element_type=jnp.float32,
                )
                made[i, parity] = total.astype(made.dtype)
            return carry

        lax.fori_loop(0, PIECE, one, 0)
        copy = pltpu.make_async_copy(made, out_ref.at[span], store_sem)
        copy.start()
        copy.wait()

    def start_tables(chunk):
        for m in sides:
            table_copy(chunk, m).start()

    def send_rows(step):
        for m in order:
            first_copy(step, m).start()

    def send_chunk(chunk):
        def one(p, carry):
            for m in order:
                later_copy(chunk * pieces + p, m).start()
            return carry

        lax.fori_loop(0, pieces, one, 0)

    def project_chunk(chunk):
        def one(p, carry):
            for m in order:
                later_copy(chunk * pieces + p, m).wait_recv()
            project(chunk * pieces + p)
            return carry

        for m in sides:
            table_copy(chunk, m).wait_recv()
        lax.fori_loop(0, pieces, one, 0)

    def first_chunk():
        def landed(step, carry):
            for m in order:
                first_copy(step, m).wait_recv()
            return carry

        def one(p, carry):
            project(p)
            return carry

        for m in sides:
            table_copy(0, m).wait_recv()
        lax.fori_loop(0, blocks, landed, 0)
        lax.fori_loop(0, pieces, one, 0)

    def nothing(step):
        del step

    pick_start = 1
    pick(0, send_rows)
    start_tables(0)
    pick(pick_start, nothing)
    start_tables(1)
    send_chunk(1)

    def stage(chunk, carry):
        pick(chunk, nothing)
        start_tables(chunk)
        send_chunk(chunk)

        @pl.when(chunk == 2)
        def _():
            first_chunk()

        @pl.when(chunk > 2)
        def _():
            project_chunk(chunk - 2)

        return carry

    lax.fori_loop(2, chunks, stage, 0)
    project_chunk(chunks - 2)
    project_chunk(chunks - 1)

    def drain_first(step, carry):
        for m in order:
            first_copy(step, m).wait_send()
        return carry

    def drain_later(piece, carry):
        for m in order:
            later_copy(piece, m).wait_send()
        return carry

    def drain_tables(chunk, carry):
        for m in sides:
            table_copy(chunk, m).wait_send()
        return carry

    lax.fori_loop(0, blocks, drain_first, 0)
    lax.fori_loop(pieces, chunks * pieces, drain_later, 0)
    lax.fori_loop(0, chunks, drain_tables, 0)


def direct_body(fourier, legendre, owner):
    lat_count, lev_count = lax.axis_size("lat"), lax.axis_size("lev")
    row_count, wave_count, column_count = fourier.shape
    half_rows = legendre.shape[3]
    slot_count = wave_count // lat_count
    chunks, blocks, pieces = slot_count // GROUP, row_count // ROWS, slot_count // PIECE
    me = lax.axis_index("lat")
    placed = ranks(owner, slot_count)
    shape = (chunks, lat_count, GROUP)
    slot_ids = (
        (me ^ lax.broadcasted_iota(jnp.int32, shape, 1)) * slot_count
        + lax.broadcasted_iota(jnp.int32, shape, 0) * GROUP
        + lax.broadcasted_iota(jnp.int32, shape, 2)
    ).reshape(chunks, lat_count * GROUP)
    picks = (placed[None, None, :] == slot_ids[:, :, None]).astype(jnp.bfloat16)
    own = me * slot_count + jnp.arange(slot_count, dtype=jnp.int32)
    wave_ids = jnp.arange(wave_count, dtype=jnp.int32)
    waves = jnp.sum(jnp.where(placed[None, :] == own[:, None], wave_ids[None, :], 0), axis=1)
    dtype = jnp.bfloat16
    anywhere = pl.BlockSpec(memory_space=pl.ANY)
    made, *_ = pl.pallas_call(
        exchange,
        in_specs=[anywhere, pl.BlockSpec(memory_space=pltpu.VMEM), anywhere],
        out_specs=[anywhere] * 4,
        out_shape=[
            jax.ShapeDtypeStruct((slot_count, 2, half_rows, column_count), dtype),
            jax.ShapeDtypeStruct((lat_count, slot_count, row_count, column_count), dtype),
            jax.ShapeDtypeStruct((lat_count - 1, slot_count, row_count, column_count), dtype),
            jax.ShapeDtypeStruct((lev_count - 1, *legendre.shape), dtype),
        ],
        scratch_shapes=[
            pltpu.VMEM((2, ROWS, wave_count, column_count), dtype),
            pltpu.VMEM((lat_count * GROUP, ROWS, column_count), jnp.float32),
            pltpu.VMEM((lat_count, GROUP, ROWS, column_count), dtype),
            pltpu.VMEM((PIECE, lat_count, row_count, column_count), dtype),
            pltpu.VMEM((PIECE, 2, lev_count * row_count, half_rows), dtype),
            pltpu.VMEM((PIECE, 2, half_rows, column_count), dtype),
            pltpu.VMEM((lat_count // 2 * row_count, column_count), dtype),
            pltpu.VMEM((lat_count // 2 * row_count, column_count), dtype),
            pltpu.SemaphoreType.DMA((2,)),
            pltpu.SemaphoreType.DMA,
            pltpu.SemaphoreType.DMA((blocks, lat_count - 1)),
            pltpu.SemaphoreType.DMA((blocks, lat_count - 1)),
            pltpu.SemaphoreType.DMA((pieces, lat_count - 1)),
            pltpu.SemaphoreType.DMA((pieces, lat_count - 1)),
            pltpu.SemaphoreType.DMA((chunks, lev_count - 1)),
            pltpu.SemaphoreType.DMA((chunks, lev_count - 1)),
            pltpu.SemaphoreType.DMA((lat_count + lev_count,)),
            pltpu.SemaphoreType.DMA,
        ],
        compiler_params=pltpu.CompilerParams(
            collective_id=0, has_side_effects=True, vmem_limit_bytes=48 * 1024 * 1024
        ),
    )(fourier, picks, legendre)
    parity = jnp.arange(2, dtype=jnp.int32)
    live = (wave_count - waves[:, None] - parity[None, :] + 1) // 2
    degree = lax.broadcasted_iota(jnp.int32, made.shape, 2)
    return jnp.where(degree < live[:, :, None, None], made, jnp.zeros_like(made))


def slot_places(owner, slot_count):
    wave_count = owner.shape[0]
    wave_ids = jnp.arange(wave_count, dtype=jnp.int32)
    earlier = (owner[None, :] == owner[:, None]) & (wave_ids[None, :] < wave_ids[:, None])
    ranked = jnp.sum(earlier.astype(jnp.int32), axis=1)
    placed = owner * slot_count + ranked
    return placed[None, :] == wave_ids[:, None]


def project(base, wave_count, waves_ref, rows_ref, table_ref, *rest):
    out_ref = rest[-1]
    half_rows, column_count = out_ref.shape[2:]
    half = rows_ref.shape[0] // 2
    upper = rows_ref[:half, 0].astype(jnp.float32).reshape(-1, column_count)
    lower = rows_ref[half:, 0].astype(jnp.float32).reshape(-1, column_count)
    wave = waves_ref[base + pl.program_id(0)]
    degree = lax.broadcasted_iota(jnp.int32, (half_rows, column_count), 0)
    for parity in range(2):
        part = (upper + lower if parity == 0 else upper - lower).astype(jnp.bfloat16)
        total = lax.dot_general(
            table_ref[0, parity], part, (((0,), (0,)), ((), ())),
            preferred_element_type=jnp.float32,
        )
        live = (wave_count - wave - parity + 1) // 2
        out_ref[0, parity] = jnp.where(degree < live, total, 0.0).astype(out_ref.dtype)


def project_chunk(base, wave_count, own_waves, rows, table, previous):
    groups, chunk_slots, group_rows, column_count = rows.shape
    slot_count, _, north_count, half_rows = table.shape
    in_specs = [
        pl.BlockSpec((groups, 1, group_rows, column_count), lambda s, w: (0, s, 0, 0)),
        pl.BlockSpec((1, 2, north_count, half_rows), lambda s, w: (base + s, 0, 0, 0)),
    ]
    operands = [own_waves, rows, table]
    aliases = {}
    if previous is not None:
        in_specs.append(pl.BlockSpec(memory_space=pl.ANY))
        operands.append(previous)
        aliases = {3: 0}
    return pl.pallas_call(
        functools.partial(project, base, wave_count),
        grid_spec=pltpu.PrefetchScalarGridSpec(
            num_scalar_prefetch=1,
            grid=(chunk_slots,),
            in_specs=in_specs,
            out_specs=pl.BlockSpec(
                (1, 2, half_rows, column_count), lambda s, w: (base + s, 0, 0, 0)
            ),
        ),
        out_shape=jax.ShapeDtypeStruct(
            (slot_count, 2, half_rows, column_count), jnp.bfloat16
        ),
        input_output_aliases=aliases,
        compiler_params=pltpu.CompilerParams(vmem_limit_bytes=32 * 1024 * 1024),
        cost_estimate=pl.CostEstimate(
            flops=4 * chunk_slots * north_count * half_rows * column_count,
            bytes_accessed=2 * rows.size
            + 4 * chunk_slots * half_rows * (north_count + column_count),
            transcendentals=0,
        ),
    )(*operands)


def body(fourier, legendre, owner):
    lat_count = lax.axis_size("lat")
    row_count, wave_count, column_count = fourier.shape
    slot_count = wave_count // lat_count
    matched = slot_places(owner, slot_count)
    wave_ids = jnp.arange(wave_count, dtype=jnp.int32)
    wave_of = jnp.sum(jnp.where(matched, wave_ids[None, :], 0), axis=1)
    own_waves = lax.dynamic_slice_in_dim(wave_of, lax.axis_index("lat") * slot_count, slot_count)
    table = lax.all_gather(legendre, "lev", axis=2, tiled=True)
    picks = matched.astype(jnp.bfloat16).reshape(lat_count, slot_count, wave_count)
    chunks = CHUNKS if slot_count % CHUNKS == 0 else 1
    chunk_slots = slot_count // chunks
    result = None
    for chunk in range(chunks):
        base = chunk * chunk_slots
        pick = picks[:, base : base + chunk_slots].reshape(-1, wave_count)
        outgoing = lax.dot_general(
            pick, fourier, (((1,), (1,)), ((), ())), preferred_element_type=jnp.bfloat16
        )
        arrived = lax.all_to_all(outgoing, "lat", split_axis=0, concat_axis=0, tiled=True)
        arrived = arrived.reshape(lat_count, chunk_slots, row_count, column_count)
        if row_count % 16 != 0:
            arrived = arrived.reshape(2, lat_count // 2, chunk_slots, row_count, column_count)
            arrived = arrived.swapaxes(1, 2).reshape(2, chunk_slots, -1, column_count)
        result = project_chunk(base, wave_count, own_waves, arrived, table, result)
    return result


def direct_fits(mesh):
    counts = (mesh.shape["lat"], mesh.shape["lev"])
    return all(n & (n - 1) == 0 and 2 <= n <= 8 for n in counts) and counts[0] >= 4


def routed(mesh):
    lat_count, lev_count = mesh.shape["lat"], mesh.shape["lev"]

    def body_of(fourier, legendre, owner):
        row_count, wave_count, _ = fourier.shape
        slot_count = wave_count // lat_count
        fits = (
            direct_fits(mesh)
            and row_count % ROWS == 0
            and slot_count % GROUP == 0
            and slot_count // GROUP >= 4
            and row_count * lat_count // 2 == legendre.shape[2] * lev_count
            and legendre.shape[2] == row_count
        )
        return (direct_body if fits else body)(fourier, legendre, owner)

    return body_of


def solution(mesh):
    placed = (P("lat", None, "lev"), P("lat", None, "lev", None), P())
    return jax.shard_map(
        routed(mesh), mesh=mesh, in_specs=placed, out_specs=P("lat", None, None, "lev"),
        check_vma=False,
    )
```

```python
import functools

import jax
import jax.numpy as jnp
from jax import lax
from jax.experimental import pallas as pl
from jax.experimental.pallas import tpu as pltpu
from jax.sharding import PartitionSpec as P

CHUNKS = 2
GROUP = 8
PIECE = 2
ROWS = 16
MADE_ELEMENTS = 8 * 1024 * 1024


def ranks(owner, slot_count):
    wave_count = owner.shape[0]
    wave_ids = jnp.arange(wave_count, dtype=jnp.int32)
    earlier = (owner[None, :] == owner[:, None]) & (wave_ids[None, :] < wave_ids[:, None])
    ranked = jnp.sum(earlier.astype(jnp.int32), axis=1)
    return owner * slot_count + ranked


def flipped(index, mask):
    bit = 1
    result = index
    while bit <= mask:
        if mask & bit:
            result = result + bit * (1 - 2 * lax.rem(lax.div(index, bit), 2))
        bit *= 2
    return result


def far_first(count):
    half = count // 2
    far = [half + m for m in range(half)]
    near = [m for m in range(1, half)]
    order = sorted(far, key=lambda m: (m & 1, -m)) + sorted(near, key=lambda m: (m == 1, m))
    return order


def exchange(
    live_ref, fourier_ref, picks_ref, table_ref,
    out_ref, send_ref, land_ref, tables_ref,
    block, drawn, packed, rows, table, even, odd,
    block_sem, packed_sem, send_first, recv_first, send_sem, recv_sem,
    send_last, recv_last,
    table_send, table_recv, load_sem,
):
    lat_count, slot_count, row_count, column_count = send_ref.shape
    half_rows = table_ref.shape[3]
    lev_count = tables_ref.shape[0] + 1
    chunks = slot_count // GROUP
    blocks = row_count // ROWS
    pieces = GROUP // PIECE
    me, lev = lax.axis_index("lat"), lax.axis_index("lev")
    order = far_first(lat_count)
    peers = {m: (flipped(me, m), lev) for m in order}
    sides = {m: (me, flipped(lev, m)) for m in range(1, lev_count)}
    mesh_ids = pl.DeviceIdType.MESH

    barrier = pltpu.get_barrier_semaphore()
    for peer in [*peers.values(), *sides.values()]:
        pl.semaphore_signal(barrier, inc=1, device_id=peer, device_id_type=mesh_ids)
    first_block = pltpu.make_async_copy(
        fourier_ref.at[pl.ds(0, ROWS)], block.at[0], block_sem.at[0]
    )
    first_block.start()
    pl.semaphore_wait(barrier, len(peers) + len(sides))

    def table_copy(chunk, mask):
        span = pl.ds(chunk * GROUP, GROUP)
        return pltpu.make_async_remote_copy(
            src_ref=table_ref.at[span], dst_ref=tables_ref.at[mask - 1, span],
            send_sem=table_send.at[chunk, mask - 1], recv_sem=table_recv.at[chunk, mask - 1],
            device_id=sides[mask], device_id_type=mesh_ids,
        )

    def first_copy(step, mask):
        span = (pl.ds(0, GROUP), pl.ds(step * ROWS, ROWS))
        return pltpu.make_async_remote_copy(
            src_ref=send_ref.at[(mask, *span)], dst_ref=land_ref.at[(mask - 1, *span)],
            send_sem=send_first.at[step, mask - 1], recv_sem=recv_first.at[step, mask - 1],
            device_id=peers[mask], device_id_type=mesh_ids,
        )

    def last_copy(step, mask):
        span = pl.ds((chunks - 1) * GROUP + step * PIECE, PIECE)
        return pltpu.make_async_remote_copy(
            src_ref=send_ref.at[mask, span], dst_ref=land_ref.at[mask - 1, span],
            send_sem=send_last.at[step, mask - 1], recv_sem=recv_last.at[step, mask - 1],
            device_id=peers[mask], device_id_type=mesh_ids,
        )

    def later_copy(chunk, mask):
        span = pl.ds(chunk * GROUP, GROUP)
        return pltpu.make_async_remote_copy(
            src_ref=send_ref.at[mask, span], dst_ref=land_ref.at[mask - 1, span],
            send_sem=send_sem.at[chunk, mask - 1], recv_sem=recv_sem.at[chunk, mask - 1],
            device_id=peers[mask], device_id_type=mesh_ids,
        )

    def block_copy(step, side):
        return pltpu.make_async_copy(
            fourier_ref.at[pl.ds(step * ROWS, ROWS)], block.at[side], block_sem.at[side]
        )

    def pick(chunk, after):
        def one(step, carry):
            side = lax.rem(step, 2)

            @pl.when((step + 1 < blocks) | (chunk + 1 < chunks))
            def _():
                block_copy(lax.rem(step + 1, blocks), 1 - side).start()

            block_copy(step, side).wait()

            for r in range(ROWS):
                drawn[:, r, :] = jnp.dot(
                    picks_ref[chunk], block[side, r], preferred_element_type=jnp.float32
                )
            packed[...] = drawn[...].astype(packed.dtype).reshape(packed.shape)
            copy = pltpu.make_async_copy(
                packed,
                send_ref.at[:, pl.ds(chunk * GROUP, GROUP), pl.ds(step * ROWS, ROWS)],
                packed_sem,
            )
            copy.start()
            copy.wait()
            after(step)
            return carry

        lax.fori_loop(0, blocks, one, 0)

    def project(piece, arrive):
        span = pl.ds(piece * PIECE, PIECE)
        copies = [pltpu.make_async_copy(send_ref.at[0, span], rows.at[:, me], load_sem.at[0])]
        for m in range(lev_count):
            source = table_ref.at[span] if m == 0 else tables_ref.at[m - 1, span]
            start = pl.multiple_of((lev if m == 0 else sides[m][1]) * row_count, ROWS)
            copies.append(pltpu.make_async_copy(
                source, table.at[:, :, pl.ds(start, row_count)], load_sem.at[lat_count + m]))
        for copy in copies:
            copy.start()
        for m in [*order[lat_count // 2 :], *order[: lat_count // 2]]:
            arrive(m)
            copies.append(pltpu.make_async_copy(
                land_ref.at[m - 1, span], rows.at[:, peers[m][0]], load_sem.at[m]))
            copies[-1].start()
        for copy in copies:
            copy.wait()

        def one(i, carry):
            half = lat_count // 2
            slot = piece * PIECE + i
            upper = rows[i, :half].astype(jnp.float32).reshape(-1, column_count)
            lower = rows[i, half:].astype(jnp.float32).reshape(-1, column_count)
            even[...] = (upper + lower).astype(even.dtype)
            odd[...] = (upper - lower).astype(odd.dtype)
            degree = lax.broadcasted_iota(jnp.int32, (half_rows, column_count), 0)
            for parity, part in enumerate((even, odd)):
                total = lax.dot_general(
                    table[i, parity], part[...], (((0,), (0,)), ((), ())),
                    preferred_element_type=jnp.float32,
                )
                kept = jnp.where(degree < live_ref[slot, parity], total, 0.0)
                out_ref[slot, parity] = kept.astype(out_ref.dtype)
            return carry

        lax.fori_loop(0, PIECE, one, 0)

    def start_tables(chunk):
        for m in sides:
            table_copy(chunk, m).start()

    def send_rows(step):
        for m in order:
            first_copy(step, m).start()

    def send_chunk(chunk):
        for m in order:
            later_copy(chunk, m).start()

    def send_last_chunk():
        def one(p, carry):
            for m in order:
                last_copy(p, m).start()
            return carry

        lax.fori_loop(0, pieces, one, 0)

    def project_chunk(chunk):
        def one(p, carry):
            project(chunk * pieces + p, nothing)
            return carry

        for m in sides:
            table_copy(chunk, m).wait_recv()
        for m in order:
            later_copy(chunk, m).wait_recv()
        lax.fori_loop(0, pieces, one, 0)

    def project_last():
        def one(p, carry):
            project((chunks - 1) * pieces + p, lambda m: last_copy(p, m).wait_recv())
            return carry

        for m in sides:
            table_copy(chunks - 1, m).wait_recv()
        lax.fori_loop(0, pieces, one, 0)

    def first_chunk():
        def landed(step, carry):
            for m in order:
                first_copy(step, m).wait_recv()
            return carry

        def one(p, carry):
            project(p, nothing)
            return carry

        for m in sides:
            table_copy(0, m).wait_recv()
        lax.fori_loop(0, blocks, landed, 0)
        lax.fori_loop(0, pieces, one, 0)

    def nothing(unused):
        del unused

    pick(0, send_rows)
    start_tables(0)
    pick(1, nothing)
    start_tables(1)
    send_chunk(1)

    def stage(chunk, carry):
        pick(chunk, nothing)
        start_tables(chunk)

        @pl.when(chunk < chunks - 1)
        def _():
            send_chunk(chunk)

        @pl.when(chunk == chunks - 1)
        def _():
            send_last_chunk()

        @pl.when(chunk == 2)
        def _():
            first_chunk()

        @pl.when(chunk > 2)
        def _():
            project_chunk(chunk - 2)

        return carry

    lax.fori_loop(2, chunks, stage, 0)
    project_chunk(chunks - 2)
    project_last()

    def drain_first(step, carry):
        for m in order:
            first_copy(step, m).wait_send()
        return carry

    def drain_later(chunk, carry):
        for m in order:
            later_copy(chunk, m).wait_send()
        return carry

    def drain_last(step, carry):
        for m in order:
            last_copy(step, m).wait_send()
        return carry

    def drain_tables(chunk, carry):
        for m in sides:
            table_copy(chunk, m).wait_send()
        return carry

    lax.fori_loop(0, blocks, drain_first, 0)
    lax.fori_loop(1, chunks - 1, drain_later, 0)
    lax.fori_loop(0, pieces, drain_last, 0)
    lax.fori_loop(0, chunks, drain_tables, 0)


def direct_body(fourier, legendre, owner):
    lat_count, lev_count = lax.axis_size("lat"), lax.axis_size("lev")
    row_count, wave_count, column_count = fourier.shape
    half_rows = legendre.shape[3]
    slot_count = wave_count // lat_count
    chunks, blocks = slot_count // GROUP, row_count // ROWS
    me = lax.axis_index("lat")
    placed = ranks(owner, slot_count)
    shape = (chunks, lat_count, GROUP)
    slot_ids = (
        (me ^ lax.broadcasted_iota(jnp.int32, shape, 1)) * slot_count
        + lax.broadcasted_iota(jnp.int32, shape, 0) * GROUP
        + lax.broadcasted_iota(jnp.int32, shape, 2)
    ).reshape(chunks, lat_count * GROUP)
    picks = (placed[None, None, :] == slot_ids[:, :, None]).astype(jnp.bfloat16)
    own = me * slot_count + jnp.arange(slot_count, dtype=jnp.int32)
    wave_ids = jnp.arange(wave_count, dtype=jnp.int32)
    waves = jnp.sum(jnp.where(placed[None, :] == own[:, None], wave_ids[None, :], 0), axis=1)
    parity = jnp.arange(2, dtype=jnp.int32)
    live = (wave_count - waves[:, None] - parity[None, :] + 1) // 2
    dtype = jnp.bfloat16
    anywhere = pl.BlockSpec(memory_space=pl.ANY)
    made, *_ = pl.pallas_call(
        exchange,
        in_specs=[
            pl.BlockSpec(memory_space=pltpu.SMEM), anywhere,
            pl.BlockSpec(memory_space=pltpu.VMEM), anywhere,
        ],
        out_specs=[pl.BlockSpec(memory_space=pltpu.VMEM), *[anywhere] * 3],
        out_shape=[
            pltpu.VMEM((slot_count, 2, half_rows, column_count), dtype),
            jax.ShapeDtypeStruct((lat_count, slot_count, row_count, column_count), dtype),
            jax.ShapeDtypeStruct((lat_count - 1, slot_count, row_count, column_count), dtype),
            jax.ShapeDtypeStruct((lev_count - 1, *legendre.shape), dtype),
        ],
        scratch_shapes=[
            pltpu.VMEM((2, ROWS, wave_count, column_count), dtype),
            pltpu.VMEM((lat_count * GROUP, ROWS, column_count), jnp.float32),
            pltpu.VMEM((lat_count, GROUP, ROWS, column_count), dtype),
            pltpu.VMEM((PIECE, lat_count, row_count, column_count), dtype),
            pltpu.VMEM((PIECE, 2, lev_count * row_count, half_rows), dtype),
            pltpu.VMEM((lat_count // 2 * row_count, column_count), dtype),
            pltpu.VMEM((lat_count // 2 * row_count, column_count), dtype),
            pltpu.SemaphoreType.DMA((2,)),
            pltpu.SemaphoreType.DMA,
            pltpu.SemaphoreType.DMA((blocks, lat_count - 1)),
            pltpu.SemaphoreType.DMA((blocks, lat_count - 1)),
            pltpu.SemaphoreType.DMA((chunks, lat_count - 1)),
            pltpu.SemaphoreType.DMA((chunks, lat_count - 1)),
            pltpu.SemaphoreType.DMA((GROUP // PIECE, lat_count - 1)),
            pltpu.SemaphoreType.DMA((GROUP // PIECE, lat_count - 1)),
            pltpu.SemaphoreType.DMA((chunks, lev_count - 1)),
            pltpu.SemaphoreType.DMA((chunks, lev_count - 1)),
            pltpu.SemaphoreType.DMA((lat_count + lev_count,)),
        ],
        compiler_params=pltpu.CompilerParams(
            collective_id=0, has_side_effects=True, vmem_limit_bytes=32 * 1024 * 1024
        ),
    )(live, fourier, picks, legendre)
    return made


def slot_places(owner, slot_count):
    wave_count = owner.shape[0]
    wave_ids = jnp.arange(wave_count, dtype=jnp.int32)
    earlier = (owner[None, :] == owner[:, None]) & (wave_ids[None, :] < wave_ids[:, None])
    ranked = jnp.sum(earlier.astype(jnp.int32), axis=1)
    placed = owner * slot_count + ranked
    return placed[None, :] == wave_ids[:, None]


def project(base, wave_count, waves_ref, rows_ref, table_ref, *rest):
    out_ref = rest[-1]
    half_rows, column_count = out_ref.shape[2:]
    half = rows_ref.shape[0] // 2
    upper = rows_ref[:half, 0].astype(jnp.float32).reshape(-1, column_count)
    lower = rows_ref[half:, 0].astype(jnp.float32).reshape(-1, column_count)
    wave = waves_ref[base + pl.program_id(0)]
    degree = lax.broadcasted_iota(jnp.int32, (half_rows, column_count), 0)
    for parity in range(2):
        part = (upper + lower if parity == 0 else upper - lower).astype(jnp.bfloat16)
        total = lax.dot_general(
            table_ref[0, parity], part, (((0,), (0,)), ((), ())),
            preferred_element_type=jnp.float32,
        )
        live = (wave_count - wave - parity + 1) // 2
        out_ref[0, parity] = jnp.where(degree < live, total, 0.0).astype(out_ref.dtype)


def project_chunk(base, wave_count, own_waves, rows, table, previous):
    groups, chunk_slots, group_rows, column_count = rows.shape
    slot_count, _, north_count, half_rows = table.shape
    in_specs = [
        pl.BlockSpec((groups, 1, group_rows, column_count), lambda s, w: (0, s, 0, 0)),
        pl.BlockSpec((1, 2, north_count, half_rows), lambda s, w: (base + s, 0, 0, 0)),
    ]
    operands = [own_waves, rows, table]
    aliases = {}
    if previous is not None:
        in_specs.append(pl.BlockSpec(memory_space=pl.ANY))
        operands.append(previous)
        aliases = {3: 0}
    return pl.pallas_call(
        functools.partial(project, base, wave_count),
        grid_spec=pltpu.PrefetchScalarGridSpec(
            num_scalar_prefetch=1,
            grid=(chunk_slots,),
            in_specs=in_specs,
            out_specs=pl.BlockSpec(
                (1, 2, half_rows, column_count), lambda s, w: (base + s, 0, 0, 0)
            ),
        ),
        out_shape=jax.ShapeDtypeStruct(
            (slot_count, 2, half_rows, column_count), jnp.bfloat16
        ),
        input_output_aliases=aliases,
        compiler_params=pltpu.CompilerParams(vmem_limit_bytes=32 * 1024 * 1024),
        cost_estimate=pl.CostEstimate(
            flops=4 * chunk_slots * north_count * half_rows * column_count,
            bytes_accessed=2 * rows.size
            + 4 * chunk_slots * half_rows * (north_count + column_count),
            transcendentals=0,
        ),
    )(*operands)


def body(fourier, legendre, owner):
    lat_count = lax.axis_size("lat")
    row_count, wave_count, column_count = fourier.shape
    slot_count = wave_count // lat_count
    matched = slot_places(owner, slot_count)
    wave_ids = jnp.arange(wave_count, dtype=jnp.int32)
    wave_of = jnp.sum(jnp.where(matched, wave_ids[None, :], 0), axis=1)
    own_waves = lax.dynamic_slice_in_dim(wave_of, lax.axis_index("lat") * slot_count, slot_count)
    table = lax.all_gather(legendre, "lev", axis=2, tiled=True)
    picks = matched.astype(jnp.bfloat16).reshape(lat_count, slot_count, wave_count)
    chunks = CHUNKS if slot_count % CHUNKS == 0 else 1
    chunk_slots = slot_count // chunks
    result = None
    for chunk in range(chunks):
        base = chunk * chunk_slots
        pick = picks[:, base : base + chunk_slots].reshape(-1, wave_count)
        outgoing = lax.dot_general(
            pick, fourier, (((1,), (1,)), ((), ())), preferred_element_type=jnp.bfloat16
        )
        arrived = lax.all_to_all(outgoing, "lat", split_axis=0, concat_axis=0, tiled=True)
        arrived = arrived.reshape(lat_count, chunk_slots, row_count, column_count)
        if row_count % 16 != 0:
            arrived = arrived.reshape(2, lat_count // 2, chunk_slots, row_count, column_count)
            arrived = arrived.swapaxes(1, 2).reshape(2, chunk_slots, -1, column_count)
        result = project_chunk(base, wave_count, own_waves, arrived, table, result)
    return result


def direct_fits(mesh):
    counts = (mesh.shape["lat"], mesh.shape["lev"])
    return all(n & (n - 1) == 0 and 2 <= n <= 8 for n in counts) and counts[0] >= 4


def routed(mesh):
    lat_count, lev_count = mesh.shape["lat"], mesh.shape["lev"]

    def body_of(fourier, legendre, owner):
        row_count, wave_count, _ = fourier.shape
        slot_count = wave_count // lat_count
        fits = (
            direct_fits(mesh)
            and row_count % (2 * ROWS) == 0
            and slot_count * legendre.shape[3] * fourier.shape[2] <= MADE_ELEMENTS
            and slot_count % GROUP == 0
            and slot_count // GROUP >= 4
            and row_count * lat_count // 2 == legendre.shape[2] * lev_count
            and legendre.shape[2] == row_count
        )
        return (direct_body if fits else body)(fourier, legendre, owner)

    return body_of


def solution(mesh):
    placed = (P("lat", None, "lev"), P("lat", None, "lev", None), P())
    return jax.shard_map(
        routed(mesh), mesh=mesh, in_specs=placed, out_specs=P("lat", None, None, "lev"),
        check_vma=False,
    )
```
